16 devices in a mesh: dp: 2 (over y, z), sp: 8 (over x, core).
Axes of the slice: x: 4, y: 2, z: 1, core: 2. Of those that a mesh axis runs over, the one named last changes fastest.
The devices are a block of a 4x4x8 slice.
Arguments:
- x: bfloat16 [4096, 2048], P(('dp', 'sp')), parts along dimension 0
- gain: bfloat16 [2048], replicated
- wq: bfloat16 [2048, 4096], replicated
- wk: bfloat16 [2048, 512], replicated
- wv: bfloat16 [2048, 512], replicated
- wo: bfloat16 [4096, 2048], replicated
Outputs:
- output: bfloat16 [4096, 2048], P(('dp', 'sp')), parts along dimension 0
There are 2 independent parts. The reference program is written for one: setup_inputs(seed, part) draws one part's arguments, and reference() takes and returns one part's arrays. A program takes and returns all parts, laid end to end along the dimension named above; an argument that names none is the same for every part.
All inputs are finite; a program needn't handle non-finite values.
Results may differ from the reference program's by a relative error of at most 0.012.
Values are sent between devices in bfloat16 or wider.
A program may use at most 768 MiB of HBM per device.

```python
import jax
import jax.numpy as jnp
from jax import lax

ROWS = 2048
D = 2048
HEADS = 16
KV_HEADS = 2
HEAD = 256
THETA = 10000


def setup_inputs(seed: int = 0, part: int = 0) -> dict:
    kx, kn, kq, kk, kv, ko = jax.random.split(jax.random.key(seed), 6)

    def weights(key, rows, columns):
        return jax.random.normal(key, (rows, columns), jnp.float32) * rows**-0.5

    drawn = {
        "x": jax.random.normal(jax.random.fold_in(kx, part), (ROWS, D), jnp.float32),
        "gain": 1 + 0.1 * jax.random.normal(kn, (D,), jnp.float32),
        "wq": 2 * weights(kq, D, HEADS * HEAD),
        "wk": 2 * weights(kk, D, KV_HEADS * HEAD),
        "wv": 4 * weights(kv, D, KV_HEADS * HEAD),
        "wo": weights(ko, HEADS * HEAD, D),
    }
    return {k: v.astype(jnp.bfloat16) for k, v in drawn.items()}


def normed(x, gain):
    wide = x.astype(jnp.float32)
    scale = lax.rsqrt(jnp.mean(wide * wide, -1, keepdims=True) + 1e-6)
    return (wide * scale * gain.astype(jnp.float32)).astype(jnp.bfloat16)


def turned(t, place, theta):
    half = t.shape[-1] // 2
    angle = place.astype(jnp.float32)[:, None] * theta ** (-jnp.arange(half, dtype=jnp.float32) / half)
    cos, sin = jnp.cos(angle)[:, None], jnp.sin(angle)[:, None]
    a, b = t[..., :half].astype(jnp.float32), t[..., half:].astype(jnp.float32)
    return jnp.concatenate([a * cos - b * sin, b * cos + a * sin], -1).astype(jnp.bfloat16)


def matmul(a, w):
    return jnp.dot(a, w, preferred_element_type=jnp.float32).astype(jnp.bfloat16)


def einsum(form, a, b):
    return jnp.einsum(form, a.astype(jnp.float32), b.astype(jnp.float32))


def attention(q, k, v):
    scores = einsum("tgsd,ugd->gstu", q, k) * q.shape[-1] ** -0.5
    token = jnp.arange(q.shape[0])
    scores = jnp.where(token[:, None] >= token, scores, -jnp.inf)
    weights = jax.nn.softmax(scores, -1).astype(jnp.bfloat16)
    return einsum("gstu,ugd->tgsd", weights, v).astype(jnp.bfloat16)


def reference(x, gain, wq, wk, wv, wo):
    a, place = normed(x, gain), jnp.arange(ROWS)
    q = turned(matmul(a, wq).reshape(ROWS, HEADS, HEAD), place, THETA).reshape(ROWS, KV_HEADS, -1, HEAD)
    k = turned(matmul(a, wk).reshape(ROWS, KV_HEADS, HEAD), place, THETA)
    v = matmul(a, wv).reshape(ROWS, KV_HEADS, HEAD)
    seen = attention(q, k, v).reshape(ROWS, HEADS * HEAD)
    return (x.astype(jnp.float32) + jnp.dot(seen, wo, preferred_element_type=jnp.float32)).astype(jnp.bfloat16)
```

```python
import functools

import jax
import jax.numpy as jnp
import numpy as np
from jax import lax
from jax.experimental import pallas as pl
from jax.experimental.pallas import tpu as pltpu
from jax.sharding import PartitionSpec as P

HEAD = 256
HALF = HEAD // 2
THETA = 10000
KVH = 2
HIDDEN = -1e30
COEF = HEAD**-0.5 * 1.4426950408889634
STRIP = 512
MESH = pl.DeviceIdType.MESH
BF, F32 = jnp.bfloat16, jnp.float32
K, V = 0, 1
TO_A, TO_B, TO_SIB, FWD, PASS = 0, 2, 4, 6, 7


def dot(a, b, ca, cb):
    return lax.dot_general(a, b, (((ca,), (cb,)), ((), ())), preferred_element_type=F32)


def kernel(n, x_hbm, gain_hbm, tab_hbm, off_hbm, wq_hbm, wk_hbm, wv_hbm, wo_hbm, out_hbm,
           x_s, gain_s, tab_s, off_s, a_s, wkv_s, wq_s, wo_s, q_s, kv_s, m_s, l_s, acc_s, seen_s, y_s, out_s,
           in_sem, wkv_sem, wq_sem, wo_sem, out_sem, send_sem, recv_sem):
    own = x_s.shape[0]
    width = x_s.shape[1]
    g = q_s.shape[0] // own // KVH
    rows = g * own
    qc = wq_s.shape[1] // 4
    wr = wo_s.shape[0] // 4
    nc = width // 2
    me = lax.axis_index("sp")
    c, core = me // 2, me % 2
    chips = n // 2
    sib = 2 * c + 1 - core

    def local(src, dst, sem):
        return pltpu.make_async_copy(src, dst, sem)

    ins = [local(x_hbm, x_s, in_sem.at[0]), local(gain_hbm, gain_s, in_sem.at[1]), local(tab_hbm, tab_s, in_sem.at[2]),
           local(off_hbm, off_s, in_sem.at[3])]
    wkv = [local(w.at[:, h * HEAD:(h + 1) * HEAD], wkv_s.at[h, i], wkv_sem.at[h, i])
           for h in range(KVH) for i, w in ((K, wk_hbm), (V, wv_hbm))]
    wq = lambda i: local(wq_hbm.at[:, pl.ds(i * qc, qc)], wq_s.at[:, pl.ds(i * qc, qc)], wq_sem.at[i])
    wo = lambda i: local(wo_hbm.at[pl.ds(i * wr, wr), :], wo_s.at[pl.ds(i * wr, wr), :], wo_sem.at[i])
    for d in ins + wkv[:2]:
        d.start()

    barrier = pltpu.get_barrier_semaphore()
    right, left = (me + 2) % n, (me + n - 2) % n
    for other in (sib, right, left):
        pl.semaphore_signal(barrier, inc=1, device_id={"sp": other}, device_id_type=MESH)

    def piece(h, kv, j):
        return kv_s.at[kv, h, pl.ds(j * own, own), :]

    def send(h, kv, j, to, slot):
        return pltpu.make_async_remote_copy(src_ref=piece(h, kv, j), dst_ref=piece(h, kv, j), send_sem=send_sem.at[h, slot],
                                            recv_sem=recv_sem.at[h, kv, j], device_id={"sp": to}, device_id_type=MESH)

    def arrive(h, kv, j):
        send(h, kv, j, sib, 0).wait_recv()

    def at(chip):
        return 2 * chip + core

    direct_ops = [(0, K, 1, TO_A), (0, V, 1, TO_A + 1), (0, K, 3, TO_B), (0, V, 3, TO_B + 1),
                  (1, K, 2, TO_A), (1, V, 2, TO_A + 1), (1, V, 0, TO_B + 1),
                  (2, K, 3, TO_A), (2, V, 3, TO_A + 1)]
    forward_ops = [(0, V, 1, 3, False), (1, V, 0, 2, True), (2, K, 1, 3, True), (3, K, 0, 2, True)]

    def passing(h, kv, src):
        return send(h, kv, at(src), sib, PASS + 2 * src + kv)

    def take(h, kv, src):
        arrive(h, kv, at(src))
        passing(h, kv, src).start()

    def direct(h):
        for kv in (K, V):
            send(h, kv, me, sib, TO_SIB + kv).start()
        for chip in range(3):
            @pl.when(c == chip)
            def _():
                for cc, kv, to, slot in direct_ops:
                    if cc == chip:
                        send(h, kv, me, at(to), slot).start()

    def forward(h, which):
        for chip, kv, src, to, also in forward_ops:
            if chip in which:
                @pl.when(c == chip)
                def _():
                    arrive(h, kv, at(src))
                    send(h, kv, at(src), at(to), FWD).start()
                    if also:
                        passing(h, kv, src).start()

    for d in ins:
        d.wait()
    for d in wkv[2:]:
        d.start()
    for i in range(4):
        wq(i).start()

    def norm(i, _):
        r = pl.ds(pl.multiple_of(i * 32, 32), 32)
        wide = x_s[r, :].astype(F32)
        scale = lax.rsqrt(jnp.mean(wide * wide, -1, keepdims=True) + 1e-6)
        a_s[r, :] = (wide * scale * gain_s[...].astype(F32)).astype(BF)

    lax.fori_loop(0, own // 32, norm, None)

    co, so = off_s[0, pl.ds(me, 1), :], off_s[1, pl.ds(me, 1), :]
    cb, sb = tab_s[0], tab_s[1]
    tab_s[0] = cb * co - sb * so
    tab_s[1] = sb * co + cb * so

    def turned(t):
        t = t.astype(BF).astype(F32)
        p, q = t[:, :HALF], t[:, HALF:]
        cos, sin = tab_s[0], tab_s[1]
        return jnp.concatenate([p * cos - q * sin, q * cos + p * sin], -1).astype(BF)

    mine = pl.ds(pl.multiple_of(me * own, own), own)

    def keys(h):
        wkv[2 * h].wait()
        kv_s[K, h, mine, :] = turned(dot(a_s[...], wkv_s[h, K], 1, 0))
        wkv[2 * h + 1].wait()
        kv_s[V, h, mine, :] = dot(a_s[...], wkv_s[h, V], 1, 0).astype(BF)

    keys(0)
    pl.semaphore_wait(barrier, 3)
    direct(0)
    keys(1)

    def queries(i, _):
        wq(i).wait()
        cols = pl.ds(pl.multiple_of(i * qc, qc), qc)
        t = dot(a_s[...], wq_s[:, cols], 1, 0)
        for j in range(qc // HEAD):
            q_s[pl.ds(pl.multiple_of(i * qc + j * own, own), own), :] = turned(t[:, j * HEAD:(j + 1) * HEAD])

    lax.fori_loop(0, 2, queries, None)
    for i in range(4):
        wo(i).start()

    def attend(h, j0, j1, first):
        ks = [kv_s[K, h, pl.ds(pl.multiple_of(j * own, own), own), :] for j in (j0, j1)]
        vs = [kv_s[V, h, pl.ds(pl.multiple_of(j * own, own), own), :] for j in (j0, j1)]
        steps = rows // STRIP

        def score(i):
            q = q_s[h * rows + i * STRIP:h * rows + (i + 1) * STRIP, :]
            return [dot(q, k, 1, 1) for k in ks]

        def soft(i, s):
            sl = slice(i * STRIP, (i + 1) * STRIP)
            if first:
                gap = (lax.broadcasted_iota(jnp.int32, (STRIP, own), 1) - lax.broadcasted_iota(jnp.int32, (STRIP, own), 0) % own)
                s = [jnp.where(gap + b * own <= core * own, t, HIDDEN) for b, t in enumerate(s)]
            high = jnp.max(jnp.maximum(s[0], s[1]), axis=1, keepdims=True)
            if first:
                top, keep = jnp.broadcast_to(high, (STRIP, 128)), None
            else:
                old = m_s[sl, :]
                top = jnp.maximum(old, high)
                keep = jnp.exp2((old - top) * COEF)
            m_s[sl, :] = top
            wide = jnp.concatenate([top] * (own // 128), axis=1)
            p = [jnp.exp2((t - wide) * COEF) for t in s]
            part = p[0] + p[1]
            part = sum(part[:, b * 128:(b + 1) * 128] for b in range(1, own // 128)) + part[:, :128]
            l_s[sl, :] = part if first else l_s[sl, :] * keep + part
            return [t.astype(BF) for t in p], keep

        def values(i, p, keep):
            sl = slice(i * STRIP, (i + 1) * STRIP)
            o = dot(p[0], vs[0], 1, 0) + dot(p[1], vs[1], 1, 0)
            acc_s[sl, :] = o if first else acc_s[sl, :] * jnp.concatenate([keep] * (HEAD // 128), axis=1) + o

        s, before = score(0), None
        for i in range(steps):
            ahead = score(i + 1) if i + 1 < steps else None
            p, keep = soft(i, s)
            if before is not None:
                values(*before)
            before, s = (i, p, keep), ahead
        values(*before)

    def own_chip(h):
        for kv in (K, V):
            arrive(h, kv, sib)
        attend(h, 2 * c, 2 * c + 1, True)

    def others(h):
        def step(s, _):
            @pl.when((c == 1) & (s == 0))
            def _():
                take(h, K, 0)
                for kv in (K, V):
                    arrive(h, kv, 1 - core)

            @pl.when((c == 2) & (s == 0))
            def _():
                take(h, V, 1)
                take(h, K, 0)
                take(h, V, 0)

            @pl.when((c == 3) & (s == 0))
            def _():
                take(h, K, 2)
                take(h, V, 2)
                take(h, V, 0)

            @pl.when((c >= 2) & (s == 1))
            def _():
                for kv in (K, V):
                    arrive(h, kv, 2 * (c - 1) + 1 - core)
                    arrive(h, kv, 1 - core)

            @pl.when(s == 2)
            def _():
                take(h, K, 1)
                take(h, V, 1)
                for kv in (K, V):
                    arrive(h, kv, 2 + 1 - core)

            plane = jnp.where(s == 0, core, 1 - core)
            j0 = jnp.where(s == 2, 2 + core, 2 * (c - 1) + plane)
            j1 = jnp.where(s == 2, 3 - core, jnp.where(c == 1, 1 - core, plane))
            attend(h, j0, j1, False)

        lax.fori_loop(0, c, step, None)

    def finish():
        for i in range(g):
            sl = slice(i * own, (i + 1) * own)
            total = jnp.sum(l_s[sl, :], axis=1, keepdims=True)
            seen_s[:, i * HEAD:(i + 1) * HEAD] = (acc_s[sl, :] * (1 / total)).astype(BF)

    outs = lambda i: local(out_s.at[:, pl.ds(i * nc, nc)], out_hbm.at[:, pl.ds(i * nc, nc)], out_sem.at[i])

    def project(h):
        for i in (2 * h, 2 * h + 1):
            wo(i).wait()

        def part(i, _):
            cols = pl.ds(pl.multiple_of(i * nc, nc), nc)
            y = dot(seen_s[...], wo_s[h * rows:(h + 1) * rows, cols], 1, 0)
            if h == 0:
                y_s[:, cols] = x_s[:, cols].astype(F32) + y
            else:
                out_s[:, cols] = (y_s[:, cols] + y).astype(BF)
                outs(i).start()

        lax.fori_loop(0, 2, part, None)

    own_chip(0)
    forward(0, (0, 1, 2, 3))
    direct(1)
    lax.fori_loop(2, 4, queries, None)
    others(0)
    forward(1, (0, 2, 3))
    finish()
    project(0)
    own_chip(1)
    forward(1, (1,))
    others(1)
    finish()
    project(1)

    for h in range(KVH):
        for kv in (K, V):
            send(h, kv, me, sib, TO_SIB + kv).wait_send()
        for chip in range(4):
            @pl.when(c == chip)
            def _():
                for cc, kv, to, slot in direct_ops:
                    if cc == chip:
                        send(h, kv, me, at(to), slot).wait_send()
                for cc, kv, src, to, also in forward_ops:
                    if cc == chip:
                        send(h, kv, at(src), at(to), FWD).wait_send()
                for src in range(chip):
                    for kv in (K, V):
                        passing(h, kv, src).wait_send()
    for i in range(2):
        outs(i).wait()


def solution(mesh):
    n = mesh.shape["sp"]

    def step(x, gain, wq, wk, wv, wo):
        own, width = x.shape
        freq = np.float32(THETA) ** (-np.arange(HALF, dtype=np.float32) / np.float32(HALF))
        inner = np.arange(own, dtype=np.float32)[:, None].astype(np.float64) * freq
        outer = (np.arange(n) * own)[:, None].astype(np.float64) * freq
        tab = np.stack([np.cos(inner), np.sin(inner)]).astype(np.float32)
        off = np.stack([np.cos(outer), np.sin(outer)]).astype(np.float32)
        heads = wq.shape[1] // HEAD
        rows = heads // KVH * own
        hbm = pl.BlockSpec(memory_space=pl.ANY)
        return pl.pallas_call(
            functools.partial(kernel, n),
            out_shape=jax.ShapeDtypeStruct((own, width), BF),
            in_specs=[hbm] * 8,
            out_specs=hbm,
            scratch_shapes=[
                pltpu.VMEM((own, width), BF),
                pltpu.VMEM((1, width), BF),
                pltpu.VMEM(tab.shape, F32),
                pltpu.VMEM(off.shape, F32),
                pltpu.VMEM((own, width), BF),
                pltpu.VMEM((KVH, 2, width, HEAD), BF),
                pltpu.VMEM(wq.shape, BF),
                pltpu.VMEM(wo.shape, BF),
                pltpu.VMEM((heads * own, HEAD), BF),
                pltpu.VMEM((2, KVH, n * own, HEAD), BF),
                pltpu.VMEM((rows, 128), F32),
                pltpu.VMEM((rows, 128), F32),
                pltpu.VMEM((rows, HEAD), F32),
                pltpu.VMEM((own, heads // KVH * HEAD), BF),
                pltpu.VMEM((own, width), F32),
                pltpu.VMEM((own, width), BF),
                pltpu.SemaphoreType.DMA((4,)),
                pltpu.SemaphoreType.DMA((KVH, 2)),
                pltpu.SemaphoreType.DMA((4,)),
                pltpu.SemaphoreType.DMA((4,)),
                pltpu.SemaphoreType.DMA((2,)),
                pltpu.SemaphoreType.DMA((KVH, PASS + n)),
                pltpu.SemaphoreType.DMA((KVH, 2, n)),
            ],
            compiler_params=pltpu.CompilerParams(collective_id=0, has_side_effects=True, vmem_limit_bytes=67043328),
        )(x, gain.reshape(1, width), tab, off, wq, wk, wv, wo)

    tokens, whole = P(("dp", "sp"), None), P(None, None)
    return jax.shard_map(
        step,
        mesh=mesh,
        in_specs=(tokens, P(None), whole, whole, whole, whole),
        out_specs=tokens,
        check_vma=False,
    )
```

```python
import functools

import jax
import jax.numpy as jnp
import numpy as np
from jax import lax
from jax.experimental import pallas as pl
from jax.experimental.pallas import tpu as pltpu
from jax.sharding import PartitionSpec as P

HEAD = 256
HALF = HEAD // 2
THETA = 10000
KVH = 2
HIDDEN = -1e30
COEF = HEAD**-0.5 * 1.4426950408889634
STRIP = 512
VMEM_LIMIT = 44 * 2**20
MESH = pl.DeviceIdType.MESH
BF, F32 = jnp.bfloat16, jnp.float32
K, V = 0, 1
TO_A, TO_B, TO_SIB, FWD, PASS = 0, 2, 4, 6, 7


def dot(a, b, ca, cb):
    return lax.dot_general(a, b, (((ca,), (cb,)), ((), ())), preferred_element_type=F32)


def kernel(n, x_hbm, gain_hbm, tab_hbm, off_hbm, wq_hbm, wk_hbm, wv_hbm, wo_hbm, out_s,
           x_s, gain_s, tab_s, off_s, a_s, wkv_s, w_s, q_s, kv_s, m_s, l_s, acc_s, seen_s, y_s,
           in_sem, wkv_sem, wq_sem, wo_sem, send_sem, recv_sem):
    own = x_s.shape[0]
    width = x_s.shape[1]
    g = q_s.shape[0] // own // KVH
    rows = g * own
    qc = w_s.shape[2]
    nc = qc
    me = lax.axis_index("sp")
    c, core = me // 2, me % 2
    chips = n // 2
    sib = 2 * c + 1 - core

    def local(src, dst, sem):
        return pltpu.make_async_copy(src, dst, sem)

    ins = [local(x_hbm, x_s, in_sem.at[0]), local(gain_hbm, gain_s, in_sem.at[1]), local(tab_hbm, tab_s, in_sem.at[2]),
           local(off_hbm, off_s, in_sem.at[3])]
    wkv = [local(w.at[:, h * HEAD:(h + 1) * HEAD], wkv_s.at[h, i], wkv_sem.at[h, i])
           for h in range(KVH) for i, w in ((K, wk_hbm), (V, wv_hbm))]
    wq = lambda i: local(wq_hbm.at[:, pl.ds(i * qc, qc)], w_s.at[i], wq_sem.at[i])
    wo = lambda i: local(wo_hbm.at[pl.ds(i // 2 * rows, rows), pl.ds(i % 2 * nc, nc)], w_s.at[i], wo_sem.at[i])
    for d in ins + wkv[:2]:
        d.start()

    barrier = pltpu.get_barrier_semaphore()
    right, left = (me + 2) % n, (me + n - 2) % n
    for other in (sib, right, left):
        pl.semaphore_signal(barrier, inc=1, device_id={"sp": other}, device_id_type=MESH)

    def piece(h, kv, j):
        return kv_s.at[kv, h, pl.ds(j * own, own), :]

    def send(h, kv, j, to, slot):
        return pltpu.make_async_remote_copy(src_ref=piece(h, kv, j), dst_ref=piece(h, kv, j), send_sem=send_sem.at[h, slot],
                                            recv_sem=recv_sem.at[h, kv, j], device_id={"sp": to}, device_id_type=MESH)

    def arrive(h, kv, j):
        send(h, kv, j, sib, 0).wait_recv()

    def at(chip):
        return 2 * chip + core

    direct_ops = [(0, K, 1, TO_A), (0, V, 1, TO_A + 1), (0, K, 3, TO_B), (0, V, 3, TO_B + 1),
                  (1, K, 2, TO_A), (1, V, 2, TO_A + 1), (1, V, 0, TO_B + 1),
                  (2, K, 3, TO_A), (2, V, 3, TO_A + 1)]
    forward_ops = [(0, V, 1, 3, False), (1, V, 0, 2, True), (2, K, 1, 3, True), (3, K, 0, 2, True)]

    def passing(h, kv, src):
        return send(h, kv, at(src), sib, PASS + 2 * src + kv)

    def take(h, kv, src):
        arrive(h, kv, at(src))
        passing(h, kv, src).start()

    def direct(h):
        for kv in (K, V):
            send(h, kv, me, sib, TO_SIB + kv).start()
        for chip in range(3):
            @pl.when(c == chip)
            def _():
                for cc, kv, to, slot in direct_ops:
                    if cc == chip:
                        send(h, kv, me, at(to), slot).start()

    def forward(h, which):
        for chip, kv, src, to, also in forward_ops:
            if chip in which:
                @pl.when(c == chip)
                def _():
                    arrive(h, kv, at(src))
                    send(h, kv, at(src), at(to), FWD).start()
                    if also:
                        passing(h, kv, src).start()

    for d in ins:
        d.wait()
    for d in wkv[2:] + [wq(0)]:
        d.start()

    def norm(i, _):
        r = pl.ds(pl.multiple_of(i * 32, 32), 32)
        wide = x_s[r, :].astype(F32)
        scale = lax.rsqrt(jnp.mean(wide * wide, -1, keepdims=True) + 1e-6)
        a_s[r, :] = (wide * scale * gain_s[...].astype(F32)[None]).astype(BF)

    lax.fori_loop(0, own // 32, norm, None)

    co, so = off_s[0, pl.ds(me, 1), :], off_s[1, pl.ds(me, 1), :]
    cb, sb = tab_s[0], tab_s[1]
    tab_s[0] = cb * co - sb * so
    tab_s[1] = sb * co + cb * so

    def turned(t):
        t = t.astype(BF).astype(F32)
        p, q = t[:, :HALF], t[:, HALF:]
        cos, sin = tab_s[0], tab_s[1]
        return jnp.concatenate([p * cos - q * sin, q * cos + p * sin], -1).astype(BF)

    mine = pl.ds(pl.multiple_of(me * own, own), own)

    def keys(h):
        wkv[2 * h].wait()
        kv_s[K, h, mine, :] = turned(dot(a_s[...], wkv_s[h, K], 1, 0))
        wkv[2 * h + 1].wait()
        kv_s[V, h, mine, :] = dot(a_s[...], wkv_s[h, V], 1, 0).astype(BF)

    keys(0)
    wq(1).start()
    pl.semaphore_wait(barrier, 3)
    direct(0)
    keys(1)

    def queries(i, _):
        wq(i).wait()

        @pl.when(i < 2)
        def _():
            wq(i + 2).start()

        t = dot(a_s[...], w_s[i], 1, 0)
        for j in range(qc // HEAD):
            q_s[pl.ds(pl.multiple_of(i * qc + j * own, own), own), :] = turned(t[:, j * HEAD:(j + 1) * HEAD])

    lax.fori_loop(0, 2, queries, None)

    def attend(h, j0, j1, first):
        ks = [kv_s[K, h, pl.ds(pl.multiple_of(j * own, own), own), :] for j in (j0, j1)]
        vs = [kv_s[V, h, pl.ds(pl.multiple_of(j * own, own), own), :] for j in (j0, j1)]
        steps = rows // STRIP

        def score(i):
            q = q_s[h * rows + i * STRIP:h * rows + (i + 1) * STRIP, :]
            return [dot(q, k, 1, 1) for k in ks]

        def soft(i, s):
            sl = slice(i * STRIP, (i + 1) * STRIP)
            if first:
                gap = (lax.broadcasted_iota(jnp.int32, (STRIP, own), 1) - lax.broadcasted_iota(jnp.int32, (STRIP, own), 0) % own)
                s = [jnp.where(gap + b * own <= core * own, t, HIDDEN) for b, t in enumerate(s)]
            high = jnp.max(jnp.maximum(s[0], s[1]), axis=1, keepdims=True)
            if first:
                top, keep = jnp.broadcast_to(high, (STRIP, 128)), None
            else:
                old = m_s[sl, :]
                top = jnp.maximum(old, high)
                keep = jnp.exp2((old - top) * COEF)
            m_s[sl, :] = top
            wide = jnp.concatenate([top] * (own // 128), axis=1)
            p = [jnp.exp2((t - wide) * COEF) for t in s]
            part = p[0] + p[1]
            part = sum(part[:, b * 128:(b + 1) * 128] for b in range(1, own // 128)) + part[:, :128]
            l_s[sl, :] = part if first else l_s[sl, :] * keep + part
            return [t.astype(BF) for t in p], keep

        def values(i, p, keep):
            sl = slice(i * STRIP, (i + 1) * STRIP)
            o = dot(p[0], vs[0], 1, 0) + dot(p[1], vs[1], 1, 0)
            acc_s[sl, :] = o if first else acc_s[sl, :] * jnp.concatenate([keep] * (HEAD // 128), axis=1) + o

        s, before = score(0), None
        for i in range(steps):
            ahead = score(i + 1) if i + 1 < steps else None
            p, keep = soft(i, s)
            if before is not None:
                values(*before)
            before, s = (i, p, keep), ahead
        values(*before)

    def own_chip(h):
        for kv in (K, V):
            arrive(h, kv, sib)
        attend(h, 2 * c, 2 * c + 1, True)

    def others(h):
        def step(s, _):
            @pl.when((c == 1) & (s == 0))
            def _():
                take(h, K, 0)
                for kv in (K, V):
                    arrive(h, kv, 1 - core)

            @pl.when((c == 2) & (s == 0))
            def _():
                take(h, V, 1)
                take(h, K, 0)
                take(h, V, 0)

            @pl.when((c == 3) & (s == 0))
            def _():
                take(h, K, 2)
                take(h, V, 2)
                take(h, V, 0)

            @pl.when((c >= 2) & (s == 1))
            def _():
                for kv in (K, V):
                    arrive(h, kv, 2 * (c - 1) + 1 - core)
                    arrive(h, kv, 1 - core)

            @pl.when(s == 2)
            def _():
                take(h, K, 1)
                take(h, V, 1)
                for kv in (K, V):
                    arrive(h, kv, 2 + 1 - core)

            plane = jnp.where(s == 0, core, 1 - core)
            j0 = jnp.where(s == 2, 2 + core, 2 * (c - 1) + plane)
            j1 = jnp.where(s == 2, 3 - core, jnp.where(c == 1, 1 - core, plane))
            attend(h, j0, j1, False)

        lax.fori_loop(0, c, step, None)

    def finish():
        for i in range(g):
            sl = slice(i * own, (i + 1) * own)
            total = jnp.sum(l_s[sl, :], axis=1, keepdims=True)
            seen_s[:, i * HEAD:(i + 1) * HEAD] = (acc_s[sl, :] * (1 / total)).astype(BF)

    def project(h):
        def part(i, _):
            cols = pl.ds(pl.multiple_of(i * nc, nc), nc)
            wo(2 * h + i).wait()
            y = dot(seen_s[...], w_s[2 * h + i], 1, 0)
            if h == 0:
                y_s[:, cols] = x_s[:, cols].astype(F32) + y
            else:
                out_s[:, cols] = (y_s[:, cols] + y).astype(BF)

        lax.fori_loop(0, 2, part, None)

    own_chip(0)
    forward(0, (0, 1, 2, 3))
    direct(1)
    lax.fori_loop(2, 4, queries, None)
    for i in range(4):
        wo(i).start()
    others(0)
    forward(1, (0, 2, 3))
    finish()
    project(0)
    own_chip(1)
    forward(1, (1,))
    others(1)
    finish()
    project(1)

    for h in range(KVH):
        for kv in (K, V):
            send(h, kv, me, sib, TO_SIB + kv).wait_send()
        for chip in range(4):
            @pl.when(c == chip)
            def _():
                for cc, kv, to, slot in direct_ops:
                    if cc == chip:
                        send(h, kv, me, at(to), slot).wait_send()
                for cc, kv, src, to, also in forward_ops:
                    if cc == chip:
                        send(h, kv, at(src), at(to), FWD).wait_send()
                for src in range(chip):
                    for kv in (K, V):
                        passing(h, kv, src).wait_send()


def solution(mesh):
    n = mesh.shape["sp"]

    def step(x, gain, wq, wk, wv, wo):
        own, width = x.shape
        freq = np.float32(THETA) ** (-np.arange(HALF, dtype=np.float32) / np.float32(HALF))
        inner = np.arange(own, dtype=np.float32)[:, None].astype(np.float64) * freq
        outer = (np.arange(n) * own)[:, None].astype(np.float64) * freq
        tab = np.stack([np.cos(inner), np.sin(inner)]).astype(np.float32)
        off = np.stack([np.cos(outer), np.sin(outer)]).astype(np.float32)
        heads = wq.shape[1] // HEAD
        rows = heads // KVH * own
        hbm = pl.BlockSpec(memory_space=pltpu.HBM)
        return pl.pallas_call(
            functools.partial(kernel, n),
            out_shape=jax.ShapeDtypeStruct((own, width), BF),
            in_specs=[hbm] * 8,
            out_specs=pl.BlockSpec(memory_space=pltpu.VMEM),
            scratch_shapes=[
                pltpu.VMEM((own, width), BF),
                pltpu.VMEM((width,), BF),
                pltpu.VMEM(tab.shape, F32),
                pltpu.VMEM(off.shape, F32),
                pltpu.VMEM((own, width), BF),
                pltpu.VMEM((KVH, 2, width, HEAD), BF),
                pltpu.VMEM((4, width, wq.shape[1] // 4), BF),
                pltpu.VMEM((heads * own, HEAD), BF),
                pltpu.VMEM((2, KVH, n * own, HEAD), BF),
                pltpu.VMEM((rows, 128), F32),
                pltpu.VMEM((rows, 128), F32),
                pltpu.VMEM((rows, HEAD), F32),
                pltpu.VMEM((own, heads // KVH * HEAD), BF),
                pltpu.VMEM((own, width), F32),
                pltpu.SemaphoreType.DMA((4,)),
                pltpu.SemaphoreType.DMA((KVH, 2)),
                pltpu.SemaphoreType.DMA((4,)),
                pltpu.SemaphoreType.DMA((4,)),
                pltpu.SemaphoreType.DMA((KVH, PASS + n)),
                pltpu.SemaphoreType.DMA((KVH, 2, n)),
            ],
            compiler_params=pltpu.CompilerParams(collective_id=0, has_side_effects=True, vmem_limit_bytes=VMEM_LIMIT),
        )(*(pltpu.with_memory_space_constraint(t, pltpu.HBM) for t in (x, gain, tab, off, wq, wk, wv, wo)))

    tokens, whole = P(("dp", "sp"), None), P(None, None)
    return jax.shard_map(
        step,
        mesh=mesh,
        in_specs=(tokens, P(None), whole, whole, whole, whole),
        out_specs=tokens,
        check_vma=False,
    )
```

```python
import functools

import jax
import jax.numpy as jnp
import numpy as np
from jax import lax
from jax.experimental import pallas as pl
from jax.experimental.pallas import tpu as pltpu
from jax.sharding import PartitionSpec as P

HEAD = 256
HALF = HEAD // 2
THETA = 10000
KVH = 2
HIDDEN = -1e30
COEF = HEAD**-0.5 * 1.4426950408889634
STRIP = 512
VMEM_LIMIT = 50 * 2**20
MESH = pl.DeviceIdType.MESH
BF, F32 = jnp.bfloat16, jnp.float32
K, V = 0, 1
TO_A, TO_B, TO_SIB, FWD, PASS = 0, 2, 4, 6, 7


def dot(a, b, ca, cb):
    return lax.dot_general(a, b, (((ca,), (cb,)), ((), ())), preferred_element_type=F32)


def kernel(n, x_hbm, gain_hbm, tab_hbm, off_hbm, wq_hbm, wk_hbm, wv_hbm, wo_hbm, out_s,
           x_s, gain_s, tab_s, off_s, a_s, wkv_s, w_s, q_s, kv_s, m_s, l_s, acc_s, seen_s, y_s,
           in_sem, wkv_sem, wq_sem, wo_sem, send_sem, recv_sem):
    own = x_s.shape[0]
    width = x_s.shape[1]
    g = q_s.shape[0] // own // KVH
    rows = g * own
    qc = w_s.shape[2]
    nc = qc
    me = lax.axis_index("sp")
    c, core = me // 2, me % 2
    chips = n // 2
    sib = 2 * c + 1 - core

    def local(src, dst, sem):
        return pltpu.make_async_copy(src, dst, sem)

    ins = [local(x_hbm, x_s, in_sem.at[0]), local(gain_hbm, gain_s, in_sem.at[1]), local(tab_hbm, tab_s, in_sem.at[2]),
           local(off_hbm, off_s, in_sem.at[3])]
    wkv = [local(w.at[:, h * HEAD:(h + 1) * HEAD], wkv_s.at[h, i], wkv_sem.at[h, i])
           for h in range(KVH) for i, w in ((K, wk_hbm), (V, wv_hbm))]
    wq = lambda i: local(wq_hbm.at[:, pl.ds(i * qc, qc)], w_s.at[i], wq_sem.at[i])
    wo = lambda i: local(wo_hbm.at[pl.ds(i // 2 * rows, rows), pl.ds(i % 2 * nc, nc)], w_s.at[i], wo_sem.at[i])
    for d in ins + wkv[:2]:
        d.start()

    barrier = pltpu.get_barrier_semaphore()
    right, left = (me + 2) % n, (me + n - 2) % n
    for other in (sib, right, left):
        pl.semaphore_signal(barrier, inc=1, device_id={"sp": other}, device_id_type=MESH)

    def piece(h, kv, j):
        return kv_s.at[kv, h, pl.ds(j * own, own), :]

    def send(h, kv, j, to, slot):
        return pltpu.make_async_remote_copy(src_ref=piece(h, kv, j), dst_ref=piece(h, kv, j), send_sem=send_sem.at[h, slot],
                                            recv_sem=recv_sem.at[h, kv, j], device_id={"sp": to}, device_id_type=MESH)

    def arrive(h, kv, j):
        send(h, kv, j, sib, 0).wait_recv()

    def at(chip):
        return 2 * chip + core

    direct_ops = [(0, K, 1, TO_A), (0, V, 1, TO_A + 1), (0, K, 3, TO_B), (0, V, 3, TO_B + 1),
                  (1, K, 2, TO_A), (1, V, 2, TO_A + 1), (1, V, 0, TO_B + 1),
                  (2, K, 3, TO_A), (2, V, 3, TO_A + 1)]
    forward_ops = [(0, V, 1, 3, False), (1, V, 0, 2, True), (2, K, 1, 3, True), (3, K, 0, 2, True)]

    def passing(h, kv, src):
        return send(h, kv, at(src), sib, PASS + 2 * src + kv)

    def take(h, kv, src):
        arrive(h, kv, at(src))
        passing(h, kv, src).start()

    def direct(h):
        for kv in (K, V):
            send(h, kv, me, sib, TO_SIB + kv).start()
        for chip in range(3):
            @pl.when(c == chip)
            def _():
                for cc, kv, to, slot in direct_ops:
                    if cc == chip:
                        send(h, kv, me, at(to), slot).start()

    def forward(h, which):
        for chip, kv, src, to, also in forward_ops:
            if chip in which:
                @pl.when(c == chip)
                def _():
                    arrive(h, kv, at(src))
                    send(h, kv, at(src), at(to), FWD).start()
                    if also:
                        passing(h, kv, src).start()

    for d in ins:
        d.wait()
    for d in wkv[2:] + [wq(0)]:
        d.start()

    def norm(i, _):
        r = pl.ds(pl.multiple_of(i * 32, 32), 32)
        wide = x_s[r, :].astype(F32)
        scale = lax.rsqrt(jnp.mean(wide * wide, -1, keepdims=True) + 1e-6)
        a_s[r, :] = (wide * scale * gain_s[...].astype(F32)[None]).astype(BF)

    lax.fori_loop(0, own // 32, norm, None)

    co, so = off_s[0, pl.ds(me, 1), :], off_s[1, pl.ds(me, 1), :]
    cb, sb = tab_s[0], tab_s[1]
    tab_s[0] = cb * co - sb * so
    tab_s[1] = sb * co + cb * so

    def turned(t):
        t = t.astype(BF).astype(F32)
        p, q = t[:, :HALF], t[:, HALF:]
        cos, sin = tab_s[0], tab_s[1]
        return jnp.concatenate([p * cos - q * sin, q * cos + p * sin], -1).astype(BF)

    mine = pl.ds(pl.multiple_of(me * own, own), own)

    def keys(h):
        wkv[2 * h].wait()
        kv_s[K, h, mine, :] = turned(dot(a_s[...], wkv_s[h, K], 1, 0))
        wkv[2 * h + 1].wait()
        kv_s[V, h, mine, :] = dot(a_s[...], wkv_s[h, V], 1, 0).astype(BF)

    keys(0)
    wq(1).start()
    pl.semaphore_wait(barrier, 3)
    direct(0)
    keys(1)

    def queries(i, _):
        wq(i).wait()

        @pl.when(i < 2)
        def _():
            wq(i + 2).start()

        t = dot(a_s[...], w_s[i], 1, 0)
        for j in range(qc // HEAD):
            q_s[pl.ds(pl.multiple_of(i * qc + j * own, own), own), :] = turned(t[:, j * HEAD:(j + 1) * HEAD])

    lax.fori_loop(0, 2, queries, None)

    def attend(h, j0, j1, first):
        ks = [kv_s[K, h, pl.ds(pl.multiple_of(j * own, own), own), :] for j in (j0, j1)]
        vs = [kv_s[V, h, pl.ds(pl.multiple_of(j * own, own), own), :] for j in (j0, j1)]
        steps = rows // STRIP

        def score(i):
            q = q_s[h * rows + i * STRIP:h * rows + (i + 1) * STRIP, :]
            return [dot(q, k, 1, 1) for k in ks]

        def soft(i, s):
            sl = slice(i * STRIP, (i + 1) * STRIP)
            if first:
                gap = (lax.broadcasted_iota(jnp.int32, (STRIP, own), 1) - lax.broadcasted_iota(jnp.int32, (STRIP, own), 0) % own)
                s = [jnp.where(gap + b * own <= core * own, t, HIDDEN) for b, t in enumerate(s)]
            high = jnp.max(jnp.maximum(s[0], s[1]), axis=1, keepdims=True)
            if first:
                top, keep = jnp.broadcast_to(high, (STRIP, 128)), None
            else:
                old = m_s[h, sl, :]
                top = jnp.maximum(old, high)
                keep = jnp.exp2((old - top) * COEF)
            m_s[h, sl, :] = top
            wide = jnp.concatenate([top] * (own // 128), axis=1)
            p = [jnp.exp2((t - wide) * COEF) for t in s]
            part = p[0] + p[1]
            part = sum(part[:, b * 128:(b + 1) * 128] for b in range(1, own // 128)) + part[:, :128]
            l_s[h, sl, :] = part if first else l_s[h, sl, :] * keep + part
            return [t.astype(BF) for t in p], keep

        def values(i, p, keep):
            sl = slice(i * STRIP, (i + 1) * STRIP)
            o = dot(p[0], vs[0], 1, 0) + dot(p[1], vs[1], 1, 0)
            acc_s[h, sl, :] = o if first else acc_s[h, sl, :] * jnp.concatenate([keep] * (HEAD // 128), axis=1) + o

        s, before = score(0), None
        for i in range(steps):
            ahead = score(i + 1) if i + 1 < steps else None
            p, keep = soft(i, s)
            if before is not None:
                values(*before)
            before, s = (i, p, keep), ahead
        values(*before)

    def own_chip(h):
        for kv in (K, V):
            arrive(h, kv, sib)
        attend(h, 2 * c, 2 * c + 1, True)

    def step(h, s):
        @pl.when((c == 1) & (s == 0))
        def _():
            take(h, K, 0)
            for kv in (K, V):
                arrive(h, kv, 1 - core)

        @pl.when((c == 2) & (s == 0))
        def _():
            take(h, V, 1)
            take(h, K, 0)
            take(h, V, 0)

        @pl.when((c == 3) & (s == 0))
        def _():
            take(h, K, 2)
            take(h, V, 2)
            take(h, V, 0)

        @pl.when((c >= 2) & (s == 1))
        def _():
            for kv in (K, V):
                arrive(h, kv, 2 * (c - 1) + 1 - core)
                arrive(h, kv, 1 - core)

        @pl.when((c == 3) & (s == 1))
        def _():
            take(h, K, 1)
            take(h, V, 1)

        @pl.when(s == 2)
        def _():
            for kv in (K, V):
                arrive(h, kv, 2 + 1 - core)

        plane = jnp.where(s == 0, core, 1 - core)
        j0 = jnp.where(s == 2, 2 + core, 2 * (c - 1) + plane)
        j1 = jnp.where(s == 2, 3 - core, jnp.where(c == 1, 1 - core, plane))
        attend(h, j0, j1, False)

    def steps(h, first):
        lax.fori_loop(first, c, lambda s, _: step(h, s), None)

    def finish(h):
        for i in range(g):
            sl = slice(i * own, (i + 1) * own)
            total = jnp.sum(l_s[h, sl, :], axis=1, keepdims=True)
            seen_s[:, i * HEAD:(i + 1) * HEAD] = (acc_s[h, sl, :] * (1 / total)).astype(BF)

    def project(h):
        def part(i, _):
            cols = pl.ds(pl.multiple_of(i * nc, nc), nc)
            wo(2 * h + i).wait()
            y = dot(seen_s[...], w_s[2 * h + i], 1, 0)
            if h == 0:
                y_s[:, cols] = x_s[:, cols].astype(F32) + y
            else:
                out_s[:, cols] = (y_s[:, cols] + y).astype(BF)

        lax.fori_loop(0, 2, part, None)

    own_chip(0)
    forward(0, (0, 1, 2, 3))
    direct(1)
    lax.fori_loop(2, 4, queries, None)
    for i in range(4):
        wo(i).start()

    @pl.when(c > 0)
    def _():
        step(0, 0)

    own_chip(1)
    steps(0, 1)
    forward(1, (0, 2, 3))
    finish(0)
    project(0)
    forward(1, (1,))
    steps(1, 0)
    finish(1)
    project(1)

    for h in range(KVH):
        for kv in (K, V):
            send(h, kv, me, sib, TO_SIB + kv).wait_send()
        for chip in range(4):
            @pl.when(c == chip)
            def _():
                for cc, kv, to, slot in direct_ops:
                    if cc == chip:
                        send(h, kv, me, at(to), slot).wait_send()
                for cc, kv, src, to, also in forward_ops:
                    if cc == chip:
                        send(h, kv, at(src), at(to), FWD).wait_send()
                for src in range(chip):
                    for kv in (K, V):
                        passing(h, kv, src).wait_send()


def solution(mesh):
    n = mesh.shape["sp"]

    def step(x, gain, wq, wk, wv, wo):
        own, width = x.shape
        freq = np.float32(THETA) ** (-np.arange(HALF, dtype=np.float32) / np.float32(HALF))
        inner = np.arange(own, dtype=np.float32)[:, None].astype(np.float64) * freq
        outer = (np.arange(n) * own)[:, None].astype(np.float64) * freq
        tab = np.stack([np.cos(inner), np.sin(inner)]).astype(np.float32)
        off = np.stack([np.cos(outer), np.sin(outer)]).astype(np.float32)
        heads = wq.shape[1] // HEAD
        rows = heads // KVH * own
        hbm = pl.BlockSpec(memory_space=pltpu.HBM)
        return pl.pallas_call(
            functools.partial(kernel, n),
            out_shape=jax.ShapeDtypeStruct((own, width), BF),
            in_specs=[hbm] * 8,
            out_specs=pl.BlockSpec(memory_space=pltpu.VMEM),
            scratch_shapes=[
                pltpu.VMEM((own, width), BF),
                pltpu.VMEM((width,), BF),
                pltpu.VMEM(tab.shape, F32),
                pltpu.VMEM(off.shape, F32),
                pltpu.VMEM((own, width), BF),
                pltpu.VMEM((KVH, 2, width, HEAD), BF),
                pltpu.VMEM((4, width, wq.shape[1] // 4), BF),
                pltpu.VMEM((heads * own, HEAD), BF),
                pltpu.VMEM((2, KVH, n * own, HEAD), BF),
                pltpu.VMEM((KVH, rows, 128), F32),
                pltpu.VMEM((KVH, rows, 128), F32),
                pltpu.VMEM((KVH, rows, HEAD), F32),
                pltpu.VMEM((own, heads // KVH * HEAD), BF),
                pltpu.VMEM((own, width), F32),
                pltpu.SemaphoreType.DMA((4,)),
                pltpu.SemaphoreType.DMA((KVH, 2)),
                pltpu.SemaphoreType.DMA((4,)),
                pltpu.SemaphoreType.DMA((4,)),
                pltpu.SemaphoreType.DMA((KVH, PASS + n)),
                pltpu.SemaphoreType.DMA((KVH, 2, n)),
            ],
            compiler_params=pltpu.CompilerParams(collective_id=0, has_side_effects=True, vmem_limit_bytes=VMEM_LIMIT),
        )(*(pltpu.with_memory_space_constraint(t, pltpu.HBM) for t in (x, gain, tab, off, wq, wk, wv, wo)))

    tokens, whole = P(("dp", "sp"), None), P(None, None)
    return jax.shard_map(
        step,
        mesh=mesh,
        in_specs=(tokens, P(None), whole, whole, whole, whole),
        out_specs=tokens,
        check_vma=False,
    )
```

```python
import functools

import jax
import jax.numpy as jnp
import numpy as np
from jax import lax
from jax.experimental import pallas as pl
from jax.experimental.pallas import tpu as pltpu
from jax.sharding import PartitionSpec as P

HEAD = 256
HALF = HEAD // 2
THETA = 10000
KVH = 2
HIDDEN = -1e30
COEF = HEAD**-0.5 * 1.4426950408889634
STRIP = 512
VMEM_LIMIT = 50 * 2**20
MESH = pl.DeviceIdType.MESH
BF, F32 = jnp.bfloat16, jnp.float32
K, V = 0, 1
TO_A, TO_B, TO_SIB, FWD, PASS = 0, 2, 4, 6, 7


def dot(a, b, ca, cb):
    return lax.dot_general(a, b, (((ca,), (cb,)), ((), ())), preferred_element_type=F32)


def kernel(n, x_hbm, gain_hbm, tab_hbm, off_hbm, wq_hbm, wk_hbm, wv_hbm, wo_hbm, out_s,
           x_s, gain_s, tab_s, off_s, a_s, wkv_s, w_s, q_s, kv_s, m_s, l_s, acc_s, seen_s, y_s, bias_s,
           in_sem, wkv_sem, wq_sem, wo_sem, send_sem, recv_sem):
    own = x_s.shape[0]
    width = x_s.shape[1]
    g = q_s.shape[0] // own // KVH
    rows = g * own
    qc = w_s.shape[2]
    nc = qc
    me = lax.axis_index("sp")
    c, core = me // 2, me % 2
    chips = n // 2
    sib = 2 * c + 1 - core

    def local(src, dst, sem):
        return pltpu.make_async_copy(src, dst, sem)

    ins = [local(x_hbm, x_s, in_sem.at[0]), local(gain_hbm, gain_s, in_sem.at[1]), local(tab_hbm, tab_s, in_sem.at[2]),
           local(off_hbm, off_s, in_sem.at[3])]
    wkv = [local(w.at[:, h * HEAD:(h + 1) * HEAD], wkv_s.at[h, i], wkv_sem.at[h, i])
           for h in range(KVH) for i, w in ((K, wk_hbm), (V, wv_hbm))]
    wq = lambda i: local(wq_hbm.at[:, pl.ds(i * qc, qc)], w_s.at[i], wq_sem.at[i])
    wo = lambda i: local(wo_hbm.at[pl.ds(i // 2 * rows, rows), pl.ds(i % 2 * nc, nc)], w_s.at[i], wo_sem.at[i])
    for d in ins[:1] + wkv[:2] + ins[1:]:
        d.start()

    barrier = pltpu.get_barrier_semaphore()
    right, left = (me + 2) % n, (me + n - 2) % n
    for other in (sib, right, left):
        pl.semaphore_signal(barrier, inc=1, device_id={"sp": other}, device_id_type=MESH)

    def piece(h, kv, j):
        return kv_s.at[kv, h, pl.ds(j * own, own), :]

    def send(h, kv, j, to, slot):
        return pltpu.make_async_remote_copy(src_ref=piece(h, kv, j), dst_ref=piece(h, kv, j), send_sem=send_sem.at[h, slot],
                                            recv_sem=recv_sem.at[h, kv, j], device_id={"sp": to}, device_id_type=MESH)

    def arrive(h, kv, j):
        send(h, kv, j, sib, 0).wait_recv()

    def at(chip):
        return 2 * chip + core

    direct_ops = [(0, K, 1, TO_A), (0, V, 1, TO_A + 1), (0, K, 3, TO_B), (0, V, 3, TO_B + 1),
                  (1, K, 2, TO_A), (1, V, 2, TO_A + 1), (1, V, 0, TO_B + 1),
                  (2, K, 3, TO_A), (2, V, 3, TO_A + 1)]
    forward_ops = [(0, V, 1, 3, False), (1, V, 0, 2, True), (2, K, 1, 3, True), (3, K, 0, 2, True)]

    def passing(h, kv, src):
        return send(h, kv, at(src), sib, PASS + 2 * src + kv)

    def take(h, kv, src):
        arrive(h, kv, at(src))
        passing(h, kv, src).start()

    def direct(h):
        for kv in (K, V):
            send(h, kv, me, sib, TO_SIB + kv).start()
        for chip in range(3):
            @pl.when(c == chip)
            def _():
                for cc, kv, to, slot in direct_ops:
                    if cc == chip:
                        send(h, kv, me, at(to), slot).start()

    def forward(h, which):
        for chip, kv, src, to, also in forward_ops:
            if chip in which:
                @pl.when(c == chip)
                def _():
                    arrive(h, kv, at(src))
                    send(h, kv, at(src), at(to), FWD).start()
                    if also:
                        passing(h, kv, src).start()

    bias_s[...] = jnp.where(lax.broadcasted_iota(jnp.int32, (own, own), 1) > lax.broadcasted_iota(jnp.int32, (own, own), 0), HIDDEN, 0.0)

    for d in ins[1:]:
        d.wait()
    for d in wkv[2:] + [wq(0)]:
        d.start()

    co, so = off_s[0, pl.ds(me, 1), :], off_s[1, pl.ds(me, 1), :]
    cb, sb = tab_s[0], tab_s[1]
    tab_s[0] = cb * co - sb * so
    tab_s[1] = sb * co + cb * so

    ins[0].wait()
    wq(1).start()

    def norm(i, _):
        r = pl.ds(pl.multiple_of(i * 32, 32), 32)
        wide = x_s[r, :].astype(F32)
        scale = lax.rsqrt(jnp.mean(wide * wide, -1, keepdims=True) + 1e-6)
        a_s[r, :] = (wide * scale * gain_s[...].astype(F32)[None]).astype(BF)

    lax.fori_loop(0, own // 32, norm, None, unroll=4)

    def turned(t):
        t = t.astype(BF).astype(F32)
        p, q = t[:, :HALF], t[:, HALF:]
        cos, sin = tab_s[0], tab_s[1]
        return jnp.concatenate([p * cos - q * sin, q * cos + p * sin], -1).astype(BF)

    mine = pl.ds(pl.multiple_of(me * own, own), own)

    def keys(h):
        wkv[2 * h].wait()
        kv_s[K, h, mine, :] = turned(dot(a_s[...], wkv_s[h, K], 1, 0))
        wkv[2 * h + 1].wait()
        kv_s[V, h, mine, :] = dot(a_s[...], wkv_s[h, V], 1, 0).astype(BF)

    keys(0)
    pl.semaphore_wait(barrier, 3)
    direct(0)
    keys(1)

    def queries(i, _):
        wq(i).wait()

        @pl.when(i < 2)
        def _():
            wq(i + 2).start()

        t = dot(a_s[...], w_s[i], 1, 0)
        for j in range(qc // HEAD):
            q_s[pl.ds(pl.multiple_of(i * qc + j * own, own), own), :] = turned(t[:, j * HEAD:(j + 1) * HEAD])

    lax.fori_loop(0, 2, queries, None)

    def attend(h, js, first=False):
        ks, vs = ([kv_s[kv, h, pl.ds(pl.multiple_of(j * own, own), own), :] for j in js] for kv in (K, V))
        strips = rows // STRIP

        def score(i):
            q = q_s[h * rows + i * STRIP:h * rows + (i + 1) * STRIP, :]
            return [dot(q, k, 1, 1) for k in ks]

        def soft(i, s):
            sl = slice(i * STRIP, (i + 1) * STRIP)
            if first:
                s = [s[0] + jnp.concatenate([bias_s[...]] * (STRIP // own), axis=0)] + s[1:]
            high = jnp.max(functools.reduce(jnp.maximum, s), axis=1, keepdims=True)
            if first:
                top, keep = jnp.broadcast_to(high, (STRIP, 128)), None
            else:
                old = m_s[h, sl, :]
                top = jnp.maximum(old, high)
                keep = jnp.exp2((old - top) * COEF)
            m_s[h, sl, :] = top
            wide = jnp.concatenate([top] * (own // 128), axis=1)
            p = [jnp.exp2((t - wide) * COEF) for t in s]
            part = functools.reduce(jnp.add, p)
            part = functools.reduce(jnp.add, [part[:, b:b + 128] for b in range(0, own, 128)])
            l_s[h, sl, :] = part if first else l_s[h, sl, :] * keep + part
            return [t.astype(BF) for t in p], keep

        def values(i, p, keep):
            sl = slice(i * STRIP, (i + 1) * STRIP)
            o = functools.reduce(jnp.add, [dot(t, v, 1, 0) for t, v in zip(p, vs)])
            acc_s[h, sl, :] = o if first else acc_s[h, sl, :] * jnp.concatenate([keep] * (HEAD // 128), axis=1) + o

        s, before = score(0), None
        for i in range(strips):
            ahead = score(i + 1) if i + 1 < strips else None
            p, keep = soft(i, s)
            if before is not None:
                values(*before)
            before, s = (i, p, keep), ahead
        values(*before)

    def own_chip(h):
        for kv in (K, V):
            arrive(h, kv, sib)

        @pl.when(core == 0)
        def _():
            attend(h, [me], True)

        @pl.when(core == 1)
        def _():
            attend(h, [me, sib], True)

    def step(h, s):
        @pl.when((c == 1) & (s == 0))
        def _():
            take(h, K, 0)
            for kv in (K, V):
                arrive(h, kv, 1 - core)

        @pl.when((c == 2) & (s == 0))
        def _():
            take(h, V, 1)
            take(h, K, 0)
            take(h, V, 0)

        @pl.when((c == 3) & (s == 0))
        def _():
            take(h, K, 2)
            take(h, V, 2)
            take(h, V, 0)

        @pl.when((c >= 2) & (s == 1))
        def _():
            for kv in (K, V):
                arrive(h, kv, 2 * (c - 1) + 1 - core)
                arrive(h, kv, 1 - core)

        @pl.when((c == 3) & (s == 1))
        def _():
            take(h, K, 1)
            take(h, V, 1)

        @pl.when(s == 2)
        def _():
            for kv in (K, V):
                arrive(h, kv, 2 + 1 - core)

        plane = jnp.where(s == 0, core, 1 - core)
        j0 = jnp.where(s == 2, 2 + core, 2 * (c - 1) + plane)
        j1 = jnp.where(s == 2, 3 - core, jnp.where(c == 1, 1 - core, plane))
        attend(h, [j0, j1])

    def ready(h):
        @pl.when(c == 3)
        def _():
            take(h, K, 2)
            take(h, V, 2)
            take(h, V, 0)

    def big_step(h):
        @pl.when(c == 3)
        def _():
            for kv in (K, V):
                arrive(h, kv, 4 + 1 - core)
                arrive(h, kv, 1 - core)

            take(h, K, 1)
            take(h, V, 1)
            attend(h, [4 + core, core, 5 - core, 1 - core])

    def steps(h, first):
        lax.fori_loop(first, c, lambda s, _: step(h, s), None)

    def finish(h):
        for i in range(g):
            sl = slice(i * own, (i + 1) * own)
            total = jnp.sum(l_s[h, sl, :], axis=1, keepdims=True)
            seen_s[:, i * HEAD:(i + 1) * HEAD] = (acc_s[h, sl, :] * (1 / total)).astype(BF)

    def project(h, between=lambda: None):
        def part(i):
            cols = slice(i * nc, (i + 1) * nc)
            wo(2 * h + i).wait()
            y = dot(seen_s[...], w_s[2 * h + i], 1, 0)
            if h == 0:
                y_s[:, cols] = x_s[:, cols].astype(F32) + y
            else:
                out_s[:, cols] = (y_s[:, cols] + y).astype(BF)

        part(0)
        between()
        part(1)

    own_chip(0)
    forward(0, (0, 1, 2, 3))
    direct(1)
    lax.fori_loop(2, 4, queries, None)
    for i in range(4):
        wo(i).start()
    own_chip(1)
    steps(0, 0)
    forward(1, (0, 2, 3))
    finish(0)
    project(0, lambda: ready(1))
    forward(1, (1,))
    big_step(1)
    steps(1, jnp.where(c == 3, 2, 0))
    finish(1)
    project(1)

    for h in range(KVH):
        for kv in (K, V):
            send(h, kv, me, sib, TO_SIB + kv).wait_send()
        for chip in range(4):
            @pl.when(c == chip)
            def _():
                for cc, kv, to, slot in direct_ops:
                    if cc == chip:
                        send(h, kv, me, at(to), slot).wait_send()
                for cc, kv, src, to, also in forward_ops:
                    if cc == chip:
                        send(h, kv, at(src), at(to), FWD).wait_send()
                for src in range(chip):
                    for kv in (K, V):
                        passing(h, kv, src).wait_send()


def solution(mesh):
    n = mesh.shape["sp"]

    def step(x, gain, wq, wk, wv, wo):
        own, width = x.shape
        freq = np.float32(THETA) ** (-np.arange(HALF, dtype=np.float32) / np.float32(HALF))
        inner = np.arange(own, dtype=np.float32)[:, None].astype(np.float64) * freq
        outer = (np.arange(n) * own)[:, None].astype(np.float64) * freq
        tab = np.stack([np.cos(inner), np.sin(inner)]).astype(np.float32)
        off = np.stack([np.cos(outer), np.sin(outer)]).astype(np.float32)
        heads = wq.shape[1] // HEAD
        rows = heads // KVH * own
        hbm = pl.BlockSpec(memory_space=pltpu.HBM)
        return pl.pallas_call(
            functools.partial(kernel, n),
            out_shape=jax.ShapeDtypeStruct((own, width), BF),
            in_specs=[hbm] * 8,
            out_specs=pl.BlockSpec(memory_space=pltpu.VMEM),
            scratch_shapes=[
                pltpu.VMEM((own, width), BF),
                pltpu.VMEM((width,), BF),
                pltpu.VMEM(tab.shape, F32),
                pltpu.VMEM(off.shape, F32),
                pltpu.VMEM((own, width), BF),
                pltpu.VMEM((KVH, 2, width, HEAD), BF),
                pltpu.VMEM((4, width, wq.shape[1] // 4), BF),
                pltpu.VMEM((heads * own, HEAD), BF),
                pltpu.VMEM((2, KVH, n * own, HEAD), BF),
                pltpu.VMEM((KVH, rows, 128), F32),
                pltpu.VMEM((KVH, rows, 128), F32),
                pltpu.VMEM((KVH, rows, HEAD), F32),
                pltpu.VMEM((own, heads // KVH * HEAD), BF),
                pltpu.VMEM((own, width), F32),
                pltpu.VMEM((own, own), F32),
                pltpu.SemaphoreType.DMA((4,)),
                pltpu.SemaphoreType.DMA((KVH, 2)),
                pltpu.SemaphoreType.DMA((4,)),
                pltpu.SemaphoreType.DMA((4,)),
                pltpu.SemaphoreType.DMA((KVH, PASS + n)),
                pltpu.SemaphoreType.DMA((KVH, 2, n)),
            ],
            compiler_params=pltpu.CompilerParams(collective_id=0, has_side_effects=True, vmem_limit_bytes=VMEM_LIMIT),
        )(*(pltpu.with_memory_space_constraint(t, pltpu.HBM) for t in (x, gain, tab, off, wq, wk, wv, wo)))

    tokens, whole = P(("dp", "sp"), None), P(None, None)
    return jax.shard_map(
        step,
        mesh=mesh,
        in_specs=(tokens, P(None), whole, whole, whole, whole),
        out_specs=tokens,
        check_vma=False,
    )
```

```python
import functools

import jax
import jax.numpy as jnp
import numpy as np
from jax import lax
from jax.experimental import pallas as pl
from jax.experimental.pallas import tpu as pltpu
from jax.sharding import PartitionSpec as P

HEAD = 256
HALF = HEAD // 2
THETA = 10000
KVH = 2
HIDDEN = -1e30
COEF = HEAD**-0.5 * 1.4426950408889634
STRIP = 512
VMEM_LIMIT = 50 * 2**20
MESH = pl.DeviceIdType.MESH
BF, F32 = jnp.bfloat16, jnp.float32
K, V = 0, 1
TO_A, TO_B, TO_SIB, FWD, PASS = 0, 2, 4, 6, 7


def dot(a, b, ca, cb):
    return lax.dot_general(a, b, (((ca,), (cb,)), ((), ())), preferred_element_type=F32)


def kernel(n, x_hbm, gain_hbm, tab_hbm, off_hbm, wq_hbm, wk_hbm, wv_hbm, wo_hbm, out_s,
           x_s, gain_s, tab_s, off_s, a_s, wkv_s, w_s, q_s, kv_s, m_s, l_s, acc_s, seen_s, y_s, bias_s,
           in_sem, wkv_sem, wq_sem, wo_sem, send_sem, recv_sem):
    own = x_s.shape[0]
    width = x_s.shape[1]
    g = q_s.shape[0] // own // KVH
    rows = g * own
    qc = w_s.shape[2]
    nc = qc
    me = lax.axis_index("sp")
    c, core = me // 2, me % 2
    chips = n // 2
    sib = 2 * c + 1 - core

    def local(src, dst, sem):
        return pltpu.make_async_copy(src, dst, sem)

    ins = [local(x_hbm, x_s, in_sem.at[0]), local(gain_hbm, gain_s, in_sem.at[1]), local(tab_hbm, tab_s, in_sem.at[2]),
           local(off_hbm, off_s, in_sem.at[3])]
    wkv = [local(w.at[:, h * HEAD:(h + 1) * HEAD], wkv_s.at[h, i], wkv_sem.at[h, i])
           for h in range(KVH) for i, w in ((K, wk_hbm), (V, wv_hbm))]
    wq = lambda i: local(wq_hbm.at[:, pl.ds(i * qc, qc)], w_s.at[i], wq_sem.at[i])
    wo = lambda i: local(wo_hbm.at[pl.ds(i // 2 * rows, rows), pl.ds(i % 2 * nc, nc)], w_s.at[i], wo_sem.at[i])
    for d in ins[:1] + wkv[:2] + ins[1:]:
        d.start()

    barrier = pltpu.get_barrier_semaphore()
    right, left = (me + 2) % n, (me + n - 2) % n
    for other in (sib, right, left):
        pl.semaphore_signal(barrier, inc=1, device_id={"sp": other}, device_id_type=MESH)

    def piece(h, kv, j):
        return kv_s.at[kv, h, pl.ds(j * own, own), :]

    def send(h, kv, j, to, slot):
        return pltpu.make_async_remote_copy(src_ref=piece(h, kv, j), dst_ref=piece(h, kv, j), send_sem=send_sem.at[h, slot],
                                            recv_sem=recv_sem.at[h, kv, j], device_id={"sp": to}, device_id_type=MESH)

    def arrive(h, kv, j):
        send(h, kv, j, sib, 0).wait_recv()

    def at(chip):
        return 2 * chip + core

    direct_ops = [(0, K, 1, TO_A), (0, V, 1, TO_A + 1), (0, K, 3, TO_B), (0, V, 3, TO_B + 1),
                  (1, K, 2, TO_A), (1, V, 2, TO_A + 1), (1, V, 0, TO_B + 1),
                  (2, K, 3, TO_A), (2, V, 3, TO_A + 1)]
    forward_ops = [(0, V, 1, 3, False), (1, V, 0, 2, True), (2, K, 1, 3, True), (3, K, 0, 2, True)]

    def passing(h, kv, src):
        return send(h, kv, at(src), sib, PASS + 2 * src + kv)

    def take(h, kv, src):
        arrive(h, kv, at(src))
        passing(h, kv, src).start()

    def direct(h):
        for kv in (K, V):
            send(h, kv, me, sib, TO_SIB + kv).start()
        for chip in range(3):
            @pl.when(c == chip)
            def _():
                for cc, kv, to, slot in direct_ops:
                    if cc == chip:
                        send(h, kv, me, at(to), slot).start()

    def forward(h, which):
        for chip, kv, src, to, also in forward_ops:
            if chip in which:
                @pl.when(c == chip)
                def _():
                    arrive(h, kv, at(src))
                    send(h, kv, at(src), at(to), FWD).start()
                    if also:
                        passing(h, kv, src).start()

    bias_s[...] = jnp.where(lax.broadcasted_iota(jnp.int32, (own, own), 1) > lax.broadcasted_iota(jnp.int32, (own, own), 0), HIDDEN, 0.0)

    for d in ins[1:]:
        d.wait()
    for d in wkv[2:] + [wq(0)]:
        d.start()

    co, so = off_s[0, pl.ds(me, 1), :], off_s[1, pl.ds(me, 1), :]
    cb, sb = tab_s[0], tab_s[1]
    tab_s[0] = cb * co - sb * so
    tab_s[1] = sb * co + cb * so

    ins[0].wait()
    wq(1).start()

    def norm(i, _):
        r = pl.ds(pl.multiple_of(i * 32, 32), 32)
        wide = x_s[r, :].astype(F32)
        scale = lax.rsqrt(jnp.mean(wide * wide, -1, keepdims=True) + 1e-6)
        a_s[r, :] = (wide * scale * gain_s[...].astype(F32)[None]).astype(BF)

    lax.fori_loop(0, own // 32, norm, None, unroll=4)

    def turned(t):
        t = t.astype(BF).astype(F32)
        p, q = t[:, :HALF], t[:, HALF:]
        cos, sin = tab_s[0], tab_s[1]
        return jnp.concatenate([p * cos - q * sin, q * cos + p * sin], -1).astype(BF)

    mine = pl.ds(pl.multiple_of(me * own, own), own)

    def keys(h):
        wkv[2 * h].wait()
        kv_s[K, h, mine, :] = turned(dot(a_s[...], wkv_s[h, K], 1, 0))
        wkv[2 * h + 1].wait()
        kv_s[V, h, mine, :] = dot(a_s[...], wkv_s[h, V], 1, 0).astype(BF)

    keys(0)
    pl.semaphore_wait(barrier, 3)
    direct(0)
    keys(1)

    def queries(i, _):
        wq(i).wait()

        @pl.when(i < 2)
        def _():
            wq(i + 2).start()

        t = dot(a_s[...], w_s[i], 1, 0)
        for j in range(qc // HEAD):
            q_s[pl.ds(pl.multiple_of(i * qc + j * own, own), own), :] = turned(t[:, j * HEAD:(j + 1) * HEAD])

    lax.fori_loop(0, 2, queries, None)

    def attend(h, js, first=False):
        ks, vs = ([kv_s[kv, h, pl.ds(pl.multiple_of(j * own, own), own), :] for j in js] for kv in (K, V))
        strips = rows // STRIP

        def score(i):
            q = q_s[h * rows + i * STRIP:h * rows + (i + 1) * STRIP, :]
            return [dot(q, k, 1, 1) for k in ks]

        def soft(i, s):
            sl = slice(i * STRIP, (i + 1) * STRIP)
            if first:
                s = [s[0] + jnp.concatenate([bias_s[...]] * (STRIP // own), axis=0)] + s[1:]
            high = jnp.max(functools.reduce(jnp.maximum, s), axis=1, keepdims=True)
            if first:
                top, keep = jnp.broadcast_to(high, (STRIP, 128)), None
            else:
                old = m_s[h, sl, :]
                top = jnp.maximum(old, high)
                keep = jnp.exp2((old - top) * COEF)
            m_s[h, sl, :] = top
            wide = jnp.concatenate([top] * (own // 128), axis=1)
            p = [jnp.exp2((t - wide) * COEF) for t in s]
            part = functools.reduce(jnp.add, p)
            part = functools.reduce(jnp.add, [part[:, b:b + 128] for b in range(0, own, 128)])
            l_s[h, sl, :] = part if first else l_s[h, sl, :] * keep + part
            return [t.astype(BF) for t in p], keep

        def values(i, p, keep):
            sl = slice(i * STRIP, (i + 1) * STRIP)
            o = functools.reduce(jnp.add, [dot(t, v, 1, 0) for t, v in zip(p, vs)])
            acc_s[h, sl, :] = o if first else acc_s[h, sl, :] * jnp.concatenate([keep] * (HEAD // 128), axis=1) + o

        s, before = score(0), None
        for i in range(strips):
            ahead = score(i + 1) if i + 1 < strips else None
            p, keep = soft(i, s)
            if before is not None:
                values(*before)
            before, s = (i, p, keep), ahead
        values(*before)

    def own_chip(h):
        for kv in (K, V):
            arrive(h, kv, sib)

        @pl.when(core == 0)
        def _():
            attend(h, [me], True)

        @pl.when(core == 1)
        def _():
            attend(h, [me, sib], True)

    def step(h, s):
        @pl.when((c == 1) & (s == 0))
        def _():
            take(h, K, 0)
            for kv in (K, V):
                arrive(h, kv, 1 - core)

        @pl.when((c == 2) & (s == 0))
        def _():
            take(h, V, 1)
            take(h, K, 0)
            take(h, V, 0)

        @pl.when((c == 3) & (s == 0))
        def _():
            take(h, K, 2)
            take(h, V, 2)
            take(h, V, 0)

        @pl.when((c >= 2) & (s == 1))
        def _():
            for kv in (K, V):
                arrive(h, kv, 2 * (c - 1) + 1 - core)
                arrive(h, kv, 1 - core)

        @pl.when((c == 3) & (s == 1))
        def _():
            take(h, K, 1)
            take(h, V, 1)

        @pl.when(s == 2)
        def _():
            for kv in (K, V):
                arrive(h, kv, 2 + 1 - core)

        plane = jnp.where(s == 0, core, 1 - core)
        j0 = jnp.where(s == 2, 2 + core, 2 * (c - 1) + plane)
        j1 = jnp.where(s == 2, 3 - core, jnp.where(c == 1, 1 - core, plane))
        attend(h, [j0, j1])

    def ready(h):
        @pl.when(c == 3)
        def _():
            take(h, K, 2)
            take(h, V, 2)
            take(h, V, 0)

    def big_step(h):
        @pl.when(c == 3)
        def _():
            for kv in (K, V):
                arrive(h, kv, 4 + 1 - core)
                arrive(h, kv, 1 - core)

            take(h, K, 1)
            take(h, V, 1)
            attend(h, [4 + core, core, 5 - core, 1 - core])

    def steps(h, first):
        lax.fori_loop(first, c, lambda s, _: step(h, s), None)

    def finish(h):
        for i in range(g):
            sl = slice(i * own, (i + 1) * own)
            total = jnp.sum(l_s[h, sl, :], axis=1, keepdims=True)
            seen_s[:, i * HEAD:(i + 1) * HEAD] = (acc_s[h, sl, :] * (1 / total)).astype(BF)

    def project(h, between=lambda: None):
        def part(i):
            cols = slice(i * nc, (i + 1) * nc)
            y = dot(seen_s[...], w_s[2 * h + i], 1, 0)
            if h == 0:
                y_s[:, cols] = x_s[:, cols].astype(F32) + y
            else:
                out_s[:, cols] = (y_s[:, cols] + y).astype(BF)

        for i in range(2):
            wo(2 * h + i).wait()
        finish(h)
        part(0)
        between()
        part(1)

    own_chip(0)
    forward(0, (0, 1, 2, 3))
    direct(1)
    lax.fori_loop(2, 4, queries, None)
    for i in range(4):
        wo(i).start()
    own_chip(1)
    steps(0, 0)
    forward(1, (0, 2, 3))
    project(0, lambda: ready(1))
    forward(1, (1,))
    big_step(1)
    steps(1, jnp.where(c == 3, 2, 0))
    project(1)

    for h in range(KVH):
        for kv in (K, V):
            send(h, kv, me, sib, TO_SIB + kv).wait_send()
        for chip in range(4):
            @pl.when(c == chip)
            def _():
                for cc, kv, to, slot in direct_ops:
                    if cc == chip:
                        send(h, kv, me, at(to), slot).wait_send()
                for cc, kv, src, to, also in forward_ops:
                    if cc == chip:
                        send(h, kv, at(src), at(to), FWD).wait_send()
                for src in range(chip):
                    for kv in (K, V):
                        passing(h, kv, src).wait_send()


def solution(mesh):
    n = mesh.shape["sp"]

    def step(x, gain, wq, wk, wv, wo):
        own, width = x.shape
        freq = np.float32(THETA) ** (-np.arange(HALF, dtype=np.float32) / np.float32(HALF))
        inner = np.arange(own, dtype=np.float32)[:, None].astype(np.float64) * freq
        outer = (np.arange(n) * own)[:, None].astype(np.float64) * freq
        tab = np.stack([np.cos(inner), np.sin(inner)]).astype(np.float32)
        off = np.stack([np.cos(outer), np.sin(outer)]).astype(np.float32)
        heads = wq.shape[1] // HEAD
        rows = heads // KVH * own
        hbm = pl.BlockSpec(memory_space=pltpu.HBM)
        return pl.pallas_call(
            functools.partial(kernel, n),
            out_shape=jax.ShapeDtypeStruct((own, width), BF),
            in_specs=[hbm] * 8,
            out_specs=pl.BlockSpec(memory_space=pltpu.VMEM),
            scratch_shapes=[
                pltpu.VMEM((own, width), BF),
                pltpu.VMEM((width,), BF),
                pltpu.VMEM(tab.shape, F32),
                pltpu.VMEM(off.shape, F32),
                pltpu.VMEM((own, width), BF),
                pltpu.VMEM((KVH, 2, width, HEAD), BF),
                pltpu.VMEM((4, width, wq.shape[1] // 4), BF),
                pltpu.VMEM((heads * own, HEAD), BF),
                pltpu.VMEM((2, KVH, n * own, HEAD), BF),
                pltpu.VMEM((KVH, rows, 128), F32),
                pltpu.VMEM((KVH, rows, 128), F32),
                pltpu.VMEM((KVH, rows, HEAD), F32),
                pltpu.VMEM((own, heads // KVH * HEAD), BF),
                pltpu.VMEM((own, width), F32),
                pltpu.VMEM((own, own), F32),
                pltpu.SemaphoreType.DMA((4,)),
                pltpu.SemaphoreType.DMA((KVH, 2)),
                pltpu.SemaphoreType.DMA((4,)),
                pltpu.SemaphoreType.DMA((4,)),
                pltpu.SemaphoreType.DMA((KVH, PASS + n)),
                pltpu.SemaphoreType.DMA((KVH, 2, n)),
            ],
            compiler_params=pltpu.CompilerParams(collective_id=0, has_side_effects=True, vmem_limit_bytes=VMEM_LIMIT),
        )(*(pltpu.with_memory_space_constraint(t, pltpu.HBM) for t in (x, gain, tab, off, wq, wk, wv, wo)))

    tokens, whole = P(("dp", "sp"), None), P(None, None)
    return jax.shard_map(
        step,
        mesh=mesh,
        in_specs=(tokens, P(None), whole, whole, whole, whole),
        out_specs=tokens,
        check_vma=False,
    )
```
